32 devices in a mesh: section: 8 (over z, core), expert: 4 (over y, x).
Axes of the slice: x: 2, y: 2, z: 4, core: 2. Of those that a mesh axis runs over, the one named last changes fastest.
Arguments:
- state: bfloat16 [8, 512, 2048], P('section', 'expert'), may hold values from -6 to 6
- norm_gain: float32 [8, 2048], P('section'), may hold values from 0.25 to 1.75
- expert_in: bfloat16 [8, 4, 2048, 1536], P('section', 'expert'), may hold values from -0.125 to 0.125
- expert_out: bfloat16 [8, 4, 768, 2048], P('section', 'expert'), may hold values from -0.21875 to 0.21875
- route_ids: int32 [3, 8, 512, 6], P(None, 'section', 'expert'), may hold values from 0 to 63, all different within a row
- route_weights: float32 [3, 8, 512, 6], P(None, 'section', 'expert'), may hold values from 0.3 to 3
Outputs:
- state_out: bfloat16 [8, 512, 2048], P('section', 'expert')
The draws below stay inside these ranges and needn't reach their ends.
Inputs may be any that keep to these rules, and one draw needn't show every extreme that they name: `route_ids`: each token names 6 different experts.
All inputs are finite; a program needn't handle non-finite values.
Results may differ from the reference program's by a relative error of at most 0.02.
Values may be sent and summed in bfloat16 or wider, within the bound.
No kernel may reach another device: no remote copies, remote signals or barrier semaphores. Data moves between devices by JAX's collectives and lax.ppermute only.
A program may use at most 64 MiB of HBM per device.

```python
import math
from functools import partial
import jax
import jax.numpy as jnp
from jax import lax

D = 2048
ROUTED = 64
TOP = 6
FF = 768
TICKS = 3
TOK_DEV = 128
CAP = 32
EXPERTS = 4
TOKENS = 512
N_SECTION = 8
N_EXPERT = 4


def steps_of(stream_key, extent, pieces, least, high):
    gain, own = 1.0, jax.random.fold_in(stream_key, 6)
    for position, parts in pieces:
        draws = jnp.exp(jax.random.uniform(jax.random.fold_in(own, position), (parts,), jnp.float32, least / len(pieces), high / len(pieces)))
        gain = gain * jnp.repeat(draws, extent[position] // parts).reshape([-1 if axis == position else 1 for axis in range(len(extent))])
    return gain


def choose_distinct(rng, rows, count, top, lift):
    ranking = jax.random.permutation(jax.random.fold_in(rng, 1), count)
    boost = ranking
    for power in range(3):
        boost = boost * boost // count
    boost = boost * lift // count
    lots = jax.random.randint(jax.random.fold_in(rng, 2), (rows, count), 0, 4096) + boost
    fixed_rows = jax.random.permutation(jax.random.fold_in(rng, 3), rows)[jnp.arange(count) % rows]
    lots = jnp.where(jnp.arange(rows)[:, None] == fixed_rows[None, :], 1 << 14, lots)
    priority = lots * count + jnp.arange(count)
    return lax.top_k(priority.astype(jnp.int32), top)[1].astype(jnp.int32)


def noise(stream_key, extent, deviation, most, pieces=(), kind=jnp.bfloat16):
    gain = steps_of(stream_key, extent, pieces, -0.22, 0.18) if pieces else 1.0
    result = jax.random.normal(stream_key, extent, jnp.float32) * deviation * gain
    return jnp.minimum(jnp.maximum(result, -most), most).astype(kind)


def setup_inputs(seed: int = 0) -> dict:
    splits = jax.random.split(jax.random.key(seed), 7)
    state = noise(splits[0], (N_SECTION, TOKENS, D), 1.0, 6.0, ((0, 8), (1, 4)))
    norm_gain = jnp.clip(1.0 + 0.15 * jax.random.normal(splits[1], (N_SECTION, D), jnp.float32), 0.25, 1.75)
    expert_in = noise(splits[2], (N_SECTION, EXPERTS, D, 2 * FF), D ** -0.5, 0.125, ((0, 8), (1, 4)))
    expert_out = noise(splits[3], (N_SECTION, EXPERTS, FF, D), FF ** -0.5, 0.21875, ((0, 8), (1, 4)))
    route_ids = choose_distinct(splits[4], TICKS * N_SECTION * TOKENS, ROUTED, TOP, 1536).reshape((TICKS, N_SECTION, TOKENS, TOP))
    route_weights = jnp.clip(jnp.exp(math.log(3.0) - 2.3025851 * jax.random.uniform(splits[5], (TICKS, N_SECTION, TOKENS, TOP), jnp.float32) ** steps_of(splits[5], (TICKS, N_SECTION, TOKENS, TOP), ((1, 8), (2, 4)), -0.2, 0.2)), 0.3, 3.0)
    return dict(state=state, norm_gain=norm_gain, expert_in=expert_in, expert_out=expert_out, route_ids=route_ids, route_weights=route_weights)


epsilon = 1e-06

def normalize(hidden, gain_row):
    widened = hidden.astype(jnp.float32)
    rescale = lax.rsqrt(lax.optimization_barrier(jnp.mean(widened * widened, axis=-1, keepdims=True)) + epsilon)
    return (widened * rescale * gain_row).astype(jnp.bfloat16)

def slot_tables(chosen, experts, capacity):
    window = jnp.arange(experts, dtype=jnp.int32)
    choice_hits = (chosen[:, :, None] == window[None, None, :]).astype(jnp.int32)
    picked = lax.optimization_barrier(jnp.sum(choice_hits, axis=1))
    rank_table = jnp.cumsum(picked, axis=0) - picked
    kept_table = picked * (rank_table < capacity).astype(jnp.int32)
    slot_index = jnp.arange(capacity, dtype=jnp.int32)
    slot_match = kept_table[:, :, None] * (rank_table[:, :, None] == slot_index[None, None, :]).astype(jnp.int32)
    positions = jnp.arange(chosen.shape[0], dtype=jnp.int32)
    token_at = lax.optimization_barrier(jnp.sum(slot_match * positions[:, None, None], axis=0))
    filled = lax.optimization_barrier(jnp.sum(slot_match, axis=0))
    kept_hits = choice_hits * kept_table[:, None, :]
    kept_choice = lax.optimization_barrier(jnp.sum(kept_hits, axis=2))
    flat_slot = lax.optimization_barrier(jnp.sum(kept_hits * (window[None, None, :] * capacity + rank_table[:, None, :]), axis=2))
    return (token_at, filled, flat_slot, kept_choice)

def expert_forward(token_rows, inner_weight, outer_weight):
    projected = jnp.dot(token_rows, inner_weight, preferred_element_type=jnp.float32)
    hidden_units = outer_weight.shape[0]
    activated = (jax.nn.silu(projected[:, :hidden_units]) * projected[:, hidden_units:]).astype(jnp.bfloat16)
    return jnp.dot(activated, outer_weight, preferred_element_type=jnp.float32).astype(jnp.bfloat16)

def serve_expert(operands):
    arrived, inner_one, outer_one = operands
    token_rows = arrived.reshape(-1, arrived.shape[-1])
    return expert_forward(token_rows, inner_one, outer_one).reshape(arrived.shape)

def layer(operands):
    hidden, gain_row, inner_weight, outer_weight, chosen, weights = operands
    normed = normalize(hidden, gain_row).reshape(N_EXPERT, TOK_DEV, D)
    tables = jax.vmap(partial(slot_tables, experts=EXPERTS, capacity=CAP))
    token_at, filled, flat_slot, kept_choice = tables(chosen.reshape(N_EXPERT, TOK_DEV, TOP))
    taker = jax.vmap(partial(jnp.take, axis=0))
    outbound = taker(normed, token_at) * filled[:, :, :, None].astype(jnp.bfloat16)
    served = lax.map(serve_expert, (jnp.swapaxes(outbound, 0, 1), inner_weight, outer_weight))
    returned = jnp.swapaxes(served, 0, 1).reshape(N_EXPERT, EXPERTS * CAP, D)
    picked_rows = taker(returned, flat_slot)
    mixing = weights.reshape(N_EXPERT, TOK_DEV, TOP) * kept_choice.astype(weights.dtype)
    branch = jnp.einsum('btk,btkd->btd', mixing, picked_rows.astype(jnp.float32))
    return (hidden.astype(jnp.float32) + branch.reshape(TOKENS, D)).astype(jnp.bfloat16)

def reference(state, norm_gain, expert_in, expert_out, route_ids, route_weights):
    holding = state
    for tick_index in range(TICKS):
        moved = lax.map(layer, (holding, norm_gain, expert_in, expert_out, route_ids[tick_index], route_weights[tick_index]))
        holding = jnp.roll(moved, 1, axis=0)
    return holding
```

```python
import functools

import jax
import jax.numpy as jnp
from jax import lax
from jax.experimental import pallas as pl
from jax.experimental.pallas import tpu as pltpu
from jax.sharding import PartitionSpec as P

epsilon = 1e-06


VMEM = pl.BlockSpec(memory_space=pltpu.VMEM)
SMEM = pl.BlockSpec(memory_space=pltpu.SMEM)


def partner(index, offset, experts):
    if experts & (experts - 1) == 0:
        return index ^ offset
    return (index + offset) % experts


def slot_match(me, chosen, experts, capacity):
    top, tokens = chosen.shape
    slots = experts * capacity
    slot = lax.broadcasted_iota(jnp.int32, (slots, tokens), 0)
    offset = slot // capacity
    expert = partner(me, offset, experts)
    hits = [chosen[k : k + 1, :] == expert for k in range(top)]
    hit = functools.reduce(jnp.logical_or, hits)
    earlier = lax.broadcasted_iota(jnp.int32, (tokens, tokens), 0) < lax.broadcasted_iota(
        jnp.int32, (tokens, tokens), 1
    )
    rank = jnp.dot(
        hit.astype(jnp.float32).astype(jnp.bfloat16),
        earlier.astype(jnp.float32).astype(jnp.bfloat16),
        preferred_element_type=jnp.float32,
    ).astype(jnp.int32)
    return hits, jnp.logical_and(hit, rank == slot - offset * capacity)


def combine(me, carried_ref, row_refs, ids, weights):
    experts = len(row_refs)
    capacity = row_refs[0].shape[0]
    hits, match = slot_match(me, ids, experts, capacity)
    weight = jnp.zeros(match.shape, jnp.float32)
    for k, hit in enumerate(hits):
        weight += jnp.where(hit, weights[k : k + 1, :], 0.0)
    mixing = jnp.where(match, weight, 0.0).T
    high = mixing.astype(jnp.bfloat16)
    low = (mixing - high.astype(jnp.float32)).astype(jnp.bfloat16)
    rows = jnp.concatenate([ref[...] for ref in row_refs], axis=0)
    branch = jnp.dot(high, rows, preferred_element_type=jnp.float32)
    branch += jnp.dot(low, rows, preferred_element_type=jnp.float32)
    return (carried_ref[...].astype(jnp.float32) + branch).astype(jnp.bfloat16)


def dispatch(me, hidden, gain_ref, ids, out_refs):
    experts = len(out_refs)
    capacity = out_refs[0].shape[0]
    widened = hidden.astype(jnp.float32)
    rescale = lax.rsqrt(jnp.mean(widened * widened, axis=-1, keepdims=True) + epsilon)
    normed = (widened * rescale * gain_ref[...]).astype(jnp.bfloat16)
    _, match = slot_match(me, ids, experts, capacity)
    select = match.astype(jnp.float32).astype(jnp.bfloat16)
    for block, ref in enumerate(out_refs):
        part = select[block * capacity : (block + 1) * capacity, :]
        ref[...] = jnp.dot(part, normed, preferred_element_type=jnp.float32).astype(ref.dtype)


def first_kernel(experts, me_ref, hidden_ref, gain_ref, ids_ref, *out_refs):
    dispatch(me_ref[0], hidden_ref[...], gain_ref, ids_ref[0], out_refs)


def middle_kernel(experts, tick, me_ref, carried_ref, gain_ref, ids_ref, came_ids, came_w, *refs):
    row_refs, hidden_ref, out_refs = refs[:experts], refs[experts], refs[experts + 1 :]
    me = me_ref[0]
    hidden = combine(me, carried_ref, row_refs, came_ids[tick - 1], came_w[tick - 1])
    hidden_ref[...] = hidden
    dispatch(me, hidden, gain_ref, ids_ref[tick], out_refs)


def last_kernel(experts, tick, me_ref, carried_ref, came_ids, came_w, *refs):
    row_refs, hidden_ref = refs[:experts], refs[experts]
    hidden_ref[...] = combine(
        me_ref[0], carried_ref, row_refs, came_ids[tick - 1], came_w[tick - 1]
    )


def expert_kernel(experts, gate_ref, up_ref, outer_ref, *refs):
    row_refs, out_refs, rows, total = refs[:experts], refs[experts:-2], refs[-2], refs[-1]
    step = pl.program_id(0)
    capacity = row_refs[0].shape[0]

    @pl.when(step == 0)
    def _():
        for block, ref in enumerate(row_refs):
            rows[pl.ds(block * capacity, capacity), :] = ref[...]

    token_rows = rows[...]
    gate = jnp.dot(token_rows, gate_ref[...], preferred_element_type=jnp.float32)
    up = jnp.dot(token_rows, up_ref[...], preferred_element_type=jnp.float32)
    activated = (jax.nn.silu(gate) * up).astype(jnp.bfloat16)
    part = jnp.dot(activated, outer_ref[...], preferred_element_type=jnp.float32)

    @pl.when(step == 0)
    def _():
        total[...] = part

    @pl.when(step > 0)
    def _():
        total[...] += part

    @pl.when(step == pl.num_programs(0) - 1)
    def _():
        for block, ref in enumerate(out_refs):
            ref[...] = total[pl.ds(block * capacity, capacity), :].astype(ref.dtype)


def serve(row_blocks, inner_weight, outer_weight):
    experts = len(row_blocks)
    capacity, width = row_blocks[0].shape
    units = outer_weight.shape[0]
    chunk = 256 if units % 256 == 0 else units
    steps = units // chunk
    whole = pl.BlockSpec((capacity, width), lambda j: (0, 0))
    return pl.pallas_call(
        functools.partial(expert_kernel, experts),
        grid=(steps,),
        out_shape=[jax.ShapeDtypeStruct((capacity, width), jnp.bfloat16)] * experts,
        in_specs=[
            pl.BlockSpec((width, chunk), lambda j: (0, j)),
            pl.BlockSpec((width, chunk), lambda j: (0, j + steps)),
            pl.BlockSpec((chunk, width), lambda j: (j, 0)),
        ]
        + [whole] * experts,
        out_specs=[whole] * experts,
        scratch_shapes=[
            pltpu.VMEM((experts * capacity, width), jnp.bfloat16),
            pltpu.VMEM((experts * capacity, width), jnp.float32),
        ],
        compiler_params=pltpu.CompilerParams(dimension_semantics=("arbitrary",)),
        name="serve_expert",
    )(inner_weight, inner_weight, outer_weight, *row_blocks)


def on_device(state, norm_gain, expert_in, expert_out, route_ids, route_weights):
    experts = lax.axis_size("expert")
    sections = lax.axis_size("section")
    hidden = state[0]
    tokens, width = hidden.shape
    capacity = tokens // 4
    ticks = route_ids.shape[0]
    inner_weight = expert_in[0, 0]
    outer_weight = expert_out[0, 0]
    me = lax.axis_index("expert").astype(jnp.int32)[None]
    ids = jnp.transpose(route_ids[:, 0], (0, 2, 1))
    weights = jnp.transpose(route_weights[:, 0], (0, 2, 1))

    onward = [(s, (s + 1) % sections) for s in range(sections)]
    block_shape = jax.ShapeDtypeStruct((capacity, width), jnp.bfloat16)
    hidden_shape = jax.ShapeDtypeStruct((tokens, width), jnp.bfloat16)
    away = [[(b, partner(b, d, experts)) for b in range(experts)] for d in range(experts)]
    home = [
        [
            (s * experts + partner(b, d, experts), ((s + 1) % sections) * experts + b)
            for s in range(sections)
            for b in range(experts)
        ]
        for d in range(experts)
    ]

    blocks = pl.pallas_call(
        functools.partial(first_kernel, experts),
        out_shape=[block_shape] * experts,
        in_specs=[SMEM] + [VMEM] * 3,
        out_specs=[VMEM] * experts,
        name="first_dispatch",
    )(me, hidden, norm_gain, ids)
    came_ids = lax.ppermute(ids, "section", onward)
    came_weights = lax.ppermute(weights, "section", onward)
    for tick in range(1, ticks + 1):
        arrived = [blocks[0]] + [
            lax.ppermute(blocks[d], "expert", away[d]) for d in range(1, experts)
        ]
        carried = lax.ppermute(hidden, "section", onward)
        served = serve(arrived, inner_weight, outer_weight)
        returned = [
            lax.ppermute(served[d], ("section", "expert"), home[d]) for d in range(experts)
        ]
        if tick < ticks:
            hidden, *blocks = pl.pallas_call(
                functools.partial(middle_kernel, experts, tick),
                out_shape=[hidden_shape] + [block_shape] * experts,
                in_specs=[SMEM] + [VMEM] * (5 + experts),
                out_specs=[VMEM] * (1 + experts),
                name="combine_dispatch",
            )(me, carried, norm_gain, ids, came_ids, came_weights, *returned)
        else:
            hidden = pl.pallas_call(
                functools.partial(last_kernel, experts, tick),
                out_shape=hidden_shape,
                in_specs=[SMEM] + [VMEM] * (3 + experts),
                out_specs=VMEM,
                name="combine_last",
            )(me, carried, came_ids, came_weights, *returned)
    return hidden[None]


def solution(mesh):
    in_specs = (
        P("section", "expert", None),
        P("section", None),
        P("section", "expert", None, None),
        P("section", "expert", None, None),
        P(None, "section", "expert", None),
        P(None, "section", "expert", None),
    )
    out_specs = P("section", "expert", None)
    return jax.shard_map(
        on_device, mesh=mesh, in_specs=in_specs, out_specs=out_specs, check_vma=False
    )
```

```python
import functools

import jax
import jax.numpy as jnp
from jax import lax
from jax.experimental import pallas as pl
from jax.experimental.pallas import tpu as pltpu
from jax.sharding import PartitionSpec as P

epsilon = 1e-06


VMEM = pl.BlockSpec(memory_space=pltpu.VMEM)
SMEM = pl.BlockSpec(memory_space=pltpu.SMEM)


def room(slots, width):
    return 12 * 1024 * 1024 + 12 * slots * width


def partner(index, offset, experts):
    if experts & (experts - 1) == 0:
        return index ^ offset
    return (index + offset) % experts


def slot_match(me, chosen, experts, capacity):
    top, tokens = chosen.shape
    slots = experts * capacity
    slot = lax.broadcasted_iota(jnp.int32, (slots, tokens), 0)
    offset = slot // capacity
    expert = partner(me, offset, experts)
    hits = [chosen[k : k + 1, :] == expert for k in range(top)]
    hit = functools.reduce(jnp.logical_or, hits)
    earlier = lax.broadcasted_iota(jnp.int32, (tokens, tokens), 0) < lax.broadcasted_iota(
        jnp.int32, (tokens, tokens), 1
    )
    rank = jnp.dot(
        hit.astype(jnp.float32).astype(jnp.bfloat16),
        earlier.astype(jnp.float32).astype(jnp.bfloat16),
        preferred_element_type=jnp.float32,
    ).astype(jnp.int32)
    return hits, jnp.logical_and(hit, rank == slot - offset * capacity)


def combine(me, carried_ref, row_refs, ids, weights):
    experts = len(row_refs)
    capacity = row_refs[0].shape[0]
    hits, match = slot_match(me, ids, experts, capacity)
    weight = jnp.zeros(match.shape, jnp.float32)
    for k, hit in enumerate(hits):
        weight += jnp.where(hit, weights[k : k + 1, :], 0.0)
    mixing = jnp.where(match, weight, 0.0).T
    high = mixing.astype(jnp.bfloat16)
    low = (mixing - high.astype(jnp.float32)).astype(jnp.bfloat16)
    rows = jnp.concatenate([ref[...] for ref in row_refs], axis=0)
    branch = jnp.dot(high, rows, preferred_element_type=jnp.float32)
    branch += jnp.dot(low, rows, preferred_element_type=jnp.float32)
    return (carried_ref[...].astype(jnp.float32) + branch).astype(jnp.bfloat16)


def dispatch(me, hidden, gain_ref, ids, out_refs):
    experts = len(out_refs)
    capacity = out_refs[0].shape[0]
    widened = hidden.astype(jnp.float32)
    rescale = lax.rsqrt(jnp.mean(widened * widened, axis=-1, keepdims=True) + epsilon)
    normed = (widened * rescale * gain_ref[...]).astype(jnp.bfloat16)
    _, match = slot_match(me, ids, experts, capacity)
    select = match.astype(jnp.float32).astype(jnp.bfloat16)
    for block, ref in enumerate(out_refs):
        part = select[block * capacity : (block + 1) * capacity, :]
        ref[...] = jnp.dot(part, normed, preferred_element_type=jnp.float32).astype(ref.dtype)


def first_kernel(experts, me_ref, hidden_ref, gain_ref, ids_ref, *out_refs):
    dispatch(me_ref[0], hidden_ref[...], gain_ref, ids_ref[0], out_refs)


def middle_kernel(experts, tick, me_ref, carried_ref, gain_ref, ids_ref, came_ids, came_w, *refs):
    row_refs, hidden_ref, out_refs = refs[:experts], refs[experts], refs[experts + 1 :]
    me = me_ref[0]
    hidden = combine(me, carried_ref, row_refs, came_ids[tick - 1], came_w[tick - 1])
    hidden_ref[...] = hidden
    dispatch(me, hidden, gain_ref, ids_ref[tick], out_refs)


def last_kernel(experts, tick, me_ref, carried_ref, came_ids, came_w, *refs):
    row_refs, hidden_ref = refs[:experts], refs[experts]
    hidden_ref[...] = combine(
        me_ref[0], carried_ref, row_refs, came_ids[tick - 1], came_w[tick - 1]
    )


def expert_kernel(experts, gate_ref, up_ref, outer_ref, *refs):
    row_refs, out_refs, rows, total = refs[:experts], refs[experts:-2], refs[-2], refs[-1]
    step = pl.program_id(0)
    capacity = row_refs[0].shape[0]

    @pl.when(step == 0)
    def _():
        for block, ref in enumerate(row_refs):
            rows[pl.ds(block * capacity, capacity), :] = ref[...]

    token_rows = rows[...]
    gate = jnp.dot(token_rows, gate_ref[...], preferred_element_type=jnp.float32)
    up = jnp.dot(token_rows, up_ref[...], preferred_element_type=jnp.float32)
    activated = (jax.nn.silu(gate) * up).astype(jnp.bfloat16)
    part = jnp.dot(activated, outer_ref[...], preferred_element_type=jnp.float32)

    @pl.when(step == 0)
    def _():
        total[...] = part

    @pl.when(step > 0)
    def _():
        total[...] += part

    @pl.when(step == pl.num_programs(0) - 1)
    def _():
        for block, ref in enumerate(out_refs):
            ref[...] = total[pl.ds(block * capacity, capacity), :].astype(ref.dtype)


def serve(row_blocks, inner_weight, outer_weight):
    experts = len(row_blocks)
    capacity, width = row_blocks[0].shape
    units = outer_weight.shape[0]
    chunk = 256 if units % 256 == 0 else units
    steps = units // chunk
    whole = pl.BlockSpec((capacity, width), lambda j: (0, 0))
    return pl.pallas_call(
        functools.partial(expert_kernel, experts),
        grid=(steps,),
        out_shape=[jax.ShapeDtypeStruct((capacity, width), jnp.bfloat16)] * experts,
        in_specs=[
            pl.BlockSpec((width, chunk), lambda j: (0, j)),
            pl.BlockSpec((width, chunk), lambda j: (0, j + steps)),
            pl.BlockSpec((chunk, width), lambda j: (j, 0)),
        ]
        + [whole] * experts,
        out_specs=[whole] * experts,
        scratch_shapes=[
            pltpu.VMEM((experts * capacity, width), jnp.bfloat16),
            pltpu.VMEM((experts * capacity, width), jnp.float32),
        ],
        compiler_params=pltpu.CompilerParams(
            dimension_semantics=("arbitrary",), vmem_limit_bytes=2 * room(experts * capacity, width)
        ),
        name="serve_expert",
    )(inner_weight, inner_weight, outer_weight, *row_blocks)


def on_device(state, norm_gain, expert_in, expert_out, route_ids, route_weights):
    experts = lax.axis_size("expert")
    sections = lax.axis_size("section")
    hidden = state[0]
    tokens, width = hidden.shape
    capacity = tokens // 4
    ticks = route_ids.shape[0]
    inner_weight = expert_in[0, 0]
    outer_weight = expert_out[0, 0]
    me = lax.axis_index("expert").astype(jnp.int32)[None]
    ids = jnp.transpose(route_ids[:, 0], (0, 2, 1))
    weights = jnp.transpose(route_weights[:, 0], (0, 2, 1))

    onward = [(s, (s + 1) % sections) for s in range(sections)]
    block_shape = jax.ShapeDtypeStruct((capacity, width), jnp.bfloat16)
    hidden_shape = jax.ShapeDtypeStruct((tokens, width), jnp.bfloat16)
    away = [[(b, partner(b, d, experts)) for b in range(experts)] for d in range(experts)]
    home = [
        [
            (s * experts + partner(b, d, experts), ((s + 1) % sections) * experts + b)
            for s in range(sections)
            for b in range(experts)
        ]
        for d in range(experts)
    ]

    blocks = pl.pallas_call(
        functools.partial(first_kernel, experts),
        out_shape=[block_shape] * experts,
        in_specs=[SMEM] + [VMEM] * 3,
        out_specs=[VMEM] * experts,
        compiler_params=pltpu.CompilerParams(vmem_limit_bytes=room(experts * capacity, width)),
        name="first_dispatch",
    )(me, hidden, norm_gain, ids)
    came_ids = lax.ppermute(ids, "section", onward)
    came_weights = lax.ppermute(weights, "section", onward)
    for tick in range(1, ticks + 1):
        arrived = [blocks[0]] + [
            lax.ppermute(blocks[d], "expert", away[d]) for d in range(1, experts)
        ]
        carried = lax.ppermute(hidden, "section", onward)
        served = serve(arrived, inner_weight, outer_weight)
        returned = [
            lax.ppermute(served[d], ("section", "expert"), home[d]) for d in range(experts)
        ]
        if tick < ticks:
            hidden, *blocks = pl.pallas_call(
                functools.partial(middle_kernel, experts, tick),
                out_shape=[hidden_shape] + [block_shape] * experts,
                in_specs=[SMEM] + [VMEM] * (5 + experts),
                out_specs=[VMEM] * (1 + experts),
                compiler_params=pltpu.CompilerParams(vmem_limit_bytes=room(experts * capacity, width)),
                name="combine_dispatch",
            )(me, carried, norm_gain, ids, came_ids, came_weights, *returned)
        else:
            hidden = pl.pallas_call(
                functools.partial(last_kernel, experts, tick),
                out_shape=hidden_shape,
                in_specs=[SMEM] + [VMEM] * (3 + experts),
                out_specs=VMEM,
                compiler_params=pltpu.CompilerParams(vmem_limit_bytes=room(experts * capacity, width)),
                name="combine_last",
            )(me, carried, came_ids, came_weights, *returned)
    return hidden[None]


def solution(mesh):
    in_specs = (
        P("section", "expert", None),
        P("section", None),
        P("section", "expert", None, None),
        P("section", "expert", None, None),
        P(None, "section", "expert", None),
        P(None, "section", "expert", None),
    )
    out_specs = P("section", "expert", None)
    return jax.shard_map(
        on_device, mesh=mesh, in_specs=in_specs, out_specs=out_specs, check_vma=False
    )
```

```python
import functools

import jax
import jax.numpy as jnp
from jax import lax
from jax.experimental import pallas as pl
from jax.experimental.pallas import tpu as pltpu
from jax.sharding import PartitionSpec as P

epsilon = 1e-06


VMEM = pl.BlockSpec(memory_space=pltpu.VMEM)
HBM = pl.BlockSpec(memory_space=pltpu.HBM)
SMEM = pl.BlockSpec(memory_space=pltpu.SMEM)


def room(slots, width):
    return 12 * 1024 * 1024 + 12 * slots * width


def partner(index, block, experts):
    offset = experts - 1 - block
    if experts & (experts - 1) == 0:
        return index ^ offset
    return (index + offset) % experts


def slot_match(me, chosen, experts, capacity):
    top, tokens = chosen.shape
    slots = experts * capacity
    slot = lax.broadcasted_iota(jnp.int32, (slots, tokens), 0)
    block = slot // capacity
    expert = partner(me, block, experts)
    hits = [chosen[k : k + 1, :] == expert for k in range(top)]
    hit = functools.reduce(jnp.logical_or, hits)
    earlier = lax.broadcasted_iota(jnp.int32, (tokens, tokens), 0) < lax.broadcasted_iota(
        jnp.int32, (tokens, tokens), 1
    )
    rank = jnp.dot(
        hit.astype(jnp.float32).astype(jnp.bfloat16),
        earlier.astype(jnp.float32).astype(jnp.bfloat16),
        preferred_element_type=jnp.float32,
    ).astype(jnp.int32)
    return hits, jnp.logical_and(hit, rank == slot - block * capacity)


def combine(me, carried_ref, row_refs, ids, weights):
    experts = len(row_refs)
    capacity = row_refs[0].shape[0]
    hits, match = slot_match(me, ids, experts, capacity)
    weight = jnp.zeros(match.shape, jnp.float32)
    for k, hit in enumerate(hits):
        weight += jnp.where(hit, weights[k : k + 1, :], 0.0)
    mixing = jnp.where(match, weight, 0.0).T
    high = mixing.astype(jnp.bfloat16)
    low = (mixing - high.astype(jnp.float32)).astype(jnp.bfloat16)
    rows = jnp.concatenate([ref[...] for ref in row_refs], axis=0)
    branch = jnp.dot(high, rows, preferred_element_type=jnp.float32)
    branch += jnp.dot(low, rows, preferred_element_type=jnp.float32)
    return (carried_ref[...].astype(jnp.float32) + branch).astype(jnp.bfloat16)


def dispatch(me, hidden, gain_ref, ids, out_refs):
    experts = len(out_refs)
    capacity = out_refs[0].shape[0]
    widened = hidden.astype(jnp.float32)
    rescale = lax.rsqrt(jnp.mean(widened * widened, axis=-1, keepdims=True) + epsilon)
    normed = (widened * rescale * gain_ref[...]).astype(jnp.bfloat16)
    _, match = slot_match(me, ids, experts, capacity)
    select = match.astype(jnp.float32).astype(jnp.bfloat16)
    for block, ref in enumerate(out_refs):
        part = select[block * capacity : (block + 1) * capacity, :]
        ref[...] = jnp.dot(part, normed, preferred_element_type=jnp.float32).astype(ref.dtype)


def first_kernel(experts, me_ref, hidden_hbm, gain_hbm, ids_ref, *refs):
    out_refs, (hidden_ref, gain_ref, sems) = refs[:experts], refs[experts:]
    loads = [
        pltpu.make_async_copy(hidden_hbm, hidden_ref, sems.at[0]),
        pltpu.make_async_copy(gain_hbm, gain_ref, sems.at[1]),
    ]
    for load in loads:
        load.start()
    for load in loads:
        load.wait()
    dispatch(me_ref[0], hidden_ref[...], gain_ref, ids_ref[0], out_refs)


def stage_kernel(after_ref, inner_hbm, outer_hbm, inner_ref, outer_ref, sems):
    loads = [
        pltpu.make_async_copy(inner_hbm, inner_ref, sems.at[0]),
        pltpu.make_async_copy(outer_hbm, outer_ref, sems.at[1]),
    ]
    for load in loads:
        load.start()
    for load in loads:
        load.wait()


def stage(after, inner_weight, outer_weight):
    moved = 2 * (inner_weight.size + outer_weight.size) * 2
    return pl.pallas_call(
        stage_kernel,
        out_shape=[
            pltpu.VMEM(inner_weight.shape, inner_weight.dtype),
            pltpu.VMEM(outer_weight.shape, outer_weight.dtype),
        ],
        in_specs=[pl.BlockSpec(memory_space=pl.ANY)] + [HBM] * 2,
        out_specs=[VMEM] * 2,
        scratch_shapes=[pltpu.SemaphoreType.DMA((2,))],
        cost_estimate=pl.CostEstimate(
            flops=moved * 100, bytes_accessed=moved, transcendentals=0
        ),
        compiler_params=pltpu.CompilerParams(vmem_limit_bytes=moved + room(8, 8)),
        name="stage_weights",
    )(after, inner_weight, outer_weight)


def middle_kernel(experts, tick, me_ref, carried_ref, gain_ref, ids_ref, came_ids, came_w, *refs):
    row_refs, hidden_ref, out_refs = refs[:experts], refs[experts], refs[experts + 1 :]
    me = me_ref[0]
    hidden = combine(me, carried_ref, row_refs, came_ids[tick - 1], came_w[tick - 1])
    hidden_ref[...] = hidden
    dispatch(me, hidden, gain_ref, ids_ref[tick], out_refs)


def last_kernel(experts, tick, me_ref, carried_ref, came_ids, came_w, *refs):
    row_refs, hidden_ref = refs[:experts], refs[experts]
    hidden_ref[...] = combine(
        me_ref[0], carried_ref, row_refs, came_ids[tick - 1], came_w[tick - 1]
    )


def expert_kernel(experts, inner_ref, outer_ref, *refs):
    row_refs, out_refs = refs[:experts], refs[experts:]
    capacity = row_refs[0].shape[0]
    units = outer_ref.shape[0]
    chunk = 256 if units % 256 == 0 else units
    token_rows = jnp.concatenate([ref[...] for ref in row_refs], axis=0)
    parts = []
    for start in range(0, units, chunk):
        gate = jnp.dot(
            token_rows, inner_ref[:, start : start + chunk], preferred_element_type=jnp.float32
        )
        up = jnp.dot(
            token_rows,
            inner_ref[:, units + start : units + start + chunk],
            preferred_element_type=jnp.float32,
        )
        parts.append((jax.nn.silu(gate) * up).astype(jnp.bfloat16))
    activated = jnp.concatenate(parts, axis=1)
    served = jnp.dot(activated, outer_ref[...], preferred_element_type=jnp.float32)
    for block, ref in enumerate(out_refs):
        ref[...] = served[block * capacity : (block + 1) * capacity].astype(ref.dtype)


def serve(row_blocks, inner_weight, outer_weight):
    experts = len(row_blocks)
    capacity, width = row_blocks[0].shape
    held = 2 * (inner_weight.size + outer_weight.size)
    return pl.pallas_call(
        functools.partial(expert_kernel, experts),
        out_shape=[jax.ShapeDtypeStruct((capacity, width), jnp.bfloat16)] * experts,
        in_specs=[VMEM] * (2 + experts),
        out_specs=[VMEM] * experts,
        compiler_params=pltpu.CompilerParams(
            vmem_limit_bytes=held + room(experts * capacity, width)
        ),
        name="serve_expert",
    )(inner_weight, outer_weight, *row_blocks)


def on_device(state, norm_gain, expert_in, expert_out, route_ids, route_weights):
    experts = lax.axis_size("expert")
    sections = lax.axis_size("section")
    hidden = state[0]
    tokens, width = hidden.shape
    capacity = tokens // 4
    ticks = route_ids.shape[0]
    inner_weight = expert_in[0, 0]
    outer_weight = expert_out[0, 0]
    me = lax.axis_index("expert").astype(jnp.int32)[None]
    ids = jnp.transpose(route_ids[:, 0], (0, 2, 1))
    weights = jnp.transpose(route_weights[:, 0], (0, 2, 1))

    onward = [(s, (s + 1) % sections) for s in range(sections)]
    block_shape = jax.ShapeDtypeStruct((capacity, width), jnp.bfloat16)
    hidden_shape = jax.ShapeDtypeStruct((tokens, width), jnp.bfloat16)
    away = [[(b, partner(b, d, experts)) for b in range(experts)] for d in range(experts)]
    home = [
        [
            (s * experts + partner(b, d, experts), ((s + 1) % sections) * experts + b)
            for s in range(sections)
            for b in range(experts)
        ]
        for d in range(experts)
    ]

    blocks = pl.pallas_call(
        functools.partial(first_kernel, experts),
        out_shape=[block_shape] * experts,
        in_specs=[SMEM, HBM, HBM, VMEM],
        out_specs=[VMEM] * experts,
        scratch_shapes=[
            pltpu.VMEM(hidden.shape, hidden.dtype),
            pltpu.VMEM(norm_gain.shape, norm_gain.dtype),
            pltpu.SemaphoreType.DMA((2,)),
        ],
        compiler_params=pltpu.CompilerParams(vmem_limit_bytes=room(experts * capacity, width)),
        name="first_dispatch",
    )(me, hidden, norm_gain, ids)
    came_ids = lax.ppermute(ids, "section", onward)
    came_weights = lax.ppermute(weights, "section", onward)
    inner_weight, outer_weight = stage(blocks[-1], inner_weight, outer_weight)
    for tick in range(1, ticks + 1):
        arrived = [
            lax.ppermute(blocks[d], "expert", away[d]) for d in range(experts - 1)
        ] + [blocks[experts - 1]]
        carried = lax.ppermute(hidden, "section", onward)
        served = serve(arrived, inner_weight, outer_weight)
        returned = [
            lax.ppermute(served[d], ("section", "expert"), home[d]) for d in range(experts)
        ]
        if tick < ticks:
            hidden, *blocks = pl.pallas_call(
                functools.partial(middle_kernel, experts, tick),
                out_shape=[hidden_shape] + [block_shape] * experts,
                in_specs=[SMEM] + [VMEM] * (5 + experts),
                out_specs=[VMEM] * (1 + experts),
                compiler_params=pltpu.CompilerParams(vmem_limit_bytes=room(experts * capacity, width)),
                name="combine_dispatch",
            )(me, carried, norm_gain, ids, came_ids, came_weights, *returned)
        else:
            hidden = pl.pallas_call(
                functools.partial(last_kernel, experts, tick),
                out_shape=hidden_shape,
                in_specs=[SMEM] + [VMEM] * (3 + experts),
                out_specs=VMEM,
                compiler_params=pltpu.CompilerParams(vmem_limit_bytes=room(experts * capacity, width)),
                name="combine_last",
            )(me, carried, came_ids, came_weights, *returned)
    return hidden[None]


def solution(mesh):
    in_specs = (
        P("section", "expert", None),
        P("section", None),
        P("section", "expert", None, None),
        P("section", "expert", None, None),
        P(None, "section", "expert", None),
        P(None, "section", "expert", None),
    )
    out_specs = P("section", "expert", None)
    return jax.shard_map(
        on_device, mesh=mesh, in_specs=in_specs, out_specs=out_specs, check_vma=False
    )
```

```python
import functools

import jax
import jax.numpy as jnp
from jax import lax
from jax.experimental import pallas as pl
from jax.experimental.pallas import tpu as pltpu
from jax.sharding import PartitionSpec as P

epsilon = 1e-06


VMEM = pl.BlockSpec(memory_space=pltpu.VMEM)
HBM = pl.BlockSpec(memory_space=pltpu.HBM)
SMEM = pl.BlockSpec(memory_space=pltpu.SMEM)


def room(slots, width):
    return 12 * 1024 * 1024 + 12 * slots * width


def partner(index, block, experts):
    offset = experts - 1 - block
    if experts & (experts - 1) == 0:
        return index ^ offset
    return (index + offset) % experts


def slot_match(me, chosen, experts, capacity):
    top, tokens = chosen.shape
    slots = experts * capacity
    slot = lax.broadcasted_iota(jnp.int32, (slots, tokens), 0)
    block = slot // capacity
    expert = partner(me, block, experts)
    hits = [chosen[k : k + 1, :] == expert for k in range(top)]
    hit = functools.reduce(jnp.logical_or, hits)
    earlier = lax.broadcasted_iota(jnp.int32, (tokens, tokens), 0) < lax.broadcasted_iota(
        jnp.int32, (tokens, tokens), 1
    )
    rank = jnp.dot(
        hit.astype(jnp.float32).astype(jnp.bfloat16),
        earlier.astype(jnp.float32).astype(jnp.bfloat16),
        preferred_element_type=jnp.float32,
    ).astype(jnp.int32)
    return hits, jnp.logical_and(hit, rank == slot - block * capacity)


def combine(me, carried_ref, row_refs, ids, weights):
    experts = len(row_refs)
    capacity = row_refs[0].shape[0]
    hits, match = slot_match(me, ids, experts, capacity)
    weight = jnp.zeros(match.shape, jnp.float32)
    for k, hit in enumerate(hits):
        weight += jnp.where(hit, weights[k : k + 1, :], 0.0)
    mixing = jnp.where(match, weight, 0.0).T
    high = mixing.astype(jnp.bfloat16)
    low = (mixing - high.astype(jnp.float32)).astype(jnp.bfloat16)
    rows = jnp.concatenate([ref[...] for ref in row_refs], axis=0)
    branch = jnp.dot(high, rows, preferred_element_type=jnp.float32)
    branch += jnp.dot(low, rows, preferred_element_type=jnp.float32)
    return (carried_ref[...].astype(jnp.float32) + branch).astype(jnp.bfloat16)


def dispatch(me, hidden, gain_ref, ids, out_refs):
    experts = len(out_refs)
    capacity = out_refs[0].shape[0]
    widened = hidden.astype(jnp.float32)
    rescale = lax.rsqrt(jnp.mean(widened * widened, axis=-1, keepdims=True) + epsilon)
    normed = (widened * rescale * gain_ref[...]).astype(jnp.bfloat16)
    _, match = slot_match(me, ids, experts, capacity)
    select = match.astype(jnp.float32).astype(jnp.bfloat16)
    for block, ref in enumerate(out_refs):
        part = select[block * capacity : (block + 1) * capacity, :]
        ref[...] = jnp.dot(part, normed, preferred_element_type=jnp.float32).astype(ref.dtype)


def first_kernel(experts, me_ref, hidden_hbm, gain_hbm, ids_ref, *refs):
    out_refs, (hidden_ref, gain_ref, sems) = refs[:experts], refs[experts:]
    loads = [
        pltpu.make_async_copy(hidden_hbm, hidden_ref, sems.at[0]),
        pltpu.make_async_copy(gain_hbm, gain_ref, sems.at[1]),
    ]
    for load in loads:
        load.start()
    for load in loads:
        load.wait()
    dispatch(me_ref[0], hidden_ref[...], gain_ref, ids_ref[0], out_refs)


def stage_kernel(after_ref, inner_hbm, outer_hbm, inner_ref, outer_ref, sems):
    loads = [
        pltpu.make_async_copy(inner_hbm, inner_ref, sems.at[0]),
        pltpu.make_async_copy(outer_hbm, outer_ref, sems.at[1]),
    ]
    for load in loads:
        load.start()
    for load in loads:
        load.wait()


def stage(after, inner_weight, outer_weight):
    moved = 2 * (inner_weight.size + outer_weight.size) * 2
    return pl.pallas_call(
        stage_kernel,
        out_shape=[
            pltpu.VMEM(inner_weight.shape, inner_weight.dtype),
            pltpu.VMEM(outer_weight.shape, outer_weight.dtype),
        ],
        in_specs=[pl.BlockSpec(memory_space=pl.ANY)] + [HBM] * 2,
        out_specs=[VMEM] * 2,
        scratch_shapes=[pltpu.SemaphoreType.DMA((2,))],
        cost_estimate=pl.CostEstimate(
            flops=moved * 100, bytes_accessed=moved, transcendentals=0
        ),
        compiler_params=pltpu.CompilerParams(vmem_limit_bytes=moved + room(8, 8)),
        name="stage_weights",
    )(after, inner_weight, outer_weight)


def middle_kernel(experts, tick, me_ref, carried_ref, gain_ref, ids_ref, came_ids, came_w, *refs):
    row_refs, hidden_ref, out_refs = refs[:experts], refs[experts], refs[experts + 1 :]
    me = me_ref[0]
    hidden = combine(me, carried_ref, row_refs, came_ids[tick - 1], came_w[tick - 1])
    hidden_ref[...] = hidden
    dispatch(me, hidden, gain_ref, ids_ref[tick], out_refs)


def last_kernel(experts, tick, me_ref, carried_ref, came_ids, came_w, *refs):
    row_refs, hidden_ref = refs[:experts], refs[experts]
    hidden_ref[...] = combine(
        me_ref[0], carried_ref, row_refs, came_ids[tick - 1], came_w[tick - 1]
    )


def expert_kernel(experts, inner_ref, outer_ref, *refs):
    row_refs, out_refs = refs[:experts], refs[experts:]
    capacity = row_refs[0].shape[0]
    units = outer_ref.shape[0]
    chunk = 256 if units % 256 == 0 else units
    token_rows = jnp.concatenate([ref[...] for ref in row_refs], axis=0)
    parts = []
    for start in range(0, units, chunk):
        gate = jnp.dot(
            token_rows, inner_ref[:, start : start + chunk], preferred_element_type=jnp.float32
        )
        up = jnp.dot(
            token_rows,
            inner_ref[:, units + start : units + start + chunk],
            preferred_element_type=jnp.float32,
        )
        parts.append((jax.nn.silu(gate) * up).astype(jnp.bfloat16))
    activated = jnp.concatenate(parts, axis=1)
    served = jnp.dot(activated, outer_ref[...], preferred_element_type=jnp.float32)
    for block, ref in enumerate(out_refs):
        ref[...] = served[block * capacity : (block + 1) * capacity].astype(ref.dtype)


def serve(row_blocks, inner_weight, outer_weight):
    experts = len(row_blocks)
    capacity, width = row_blocks[0].shape
    held = 2 * (inner_weight.size + outer_weight.size)
    return pl.pallas_call(
        functools.partial(expert_kernel, experts),
        out_shape=[jax.ShapeDtypeStruct((capacity, width), jnp.bfloat16)] * experts,
        in_specs=[VMEM] * (2 + experts),
        out_specs=[VMEM] * experts,
        compiler_params=pltpu.CompilerParams(
            vmem_limit_bytes=held + room(experts * capacity, width)
        ),
        name="serve_expert",
    )(inner_weight, outer_weight, *row_blocks)


def on_device(state, norm_gain, expert_in, expert_out, route_ids, route_weights):
    experts = lax.axis_size("expert")
    sections = lax.axis_size("section")
    hidden = state[0]
    tokens, width = hidden.shape
    capacity = tokens // 4
    ticks = route_ids.shape[0]
    inner_weight = expert_in[0, 0]
    outer_weight = expert_out[0, 0]
    me = lax.axis_index("expert").astype(jnp.int32)[None]
    ids = jnp.transpose(route_ids[:, 0], (0, 2, 1))
    weights = jnp.transpose(route_weights[:, 0], (0, 2, 1))

    onward = [(s, (s + 1) % sections) for s in range(sections)]
    block_shape = jax.ShapeDtypeStruct((capacity, width), jnp.bfloat16)
    hidden_shape = jax.ShapeDtypeStruct((tokens, width), jnp.bfloat16)
    away = [[(b, partner(b, d, experts)) for b in range(experts)] for d in range(experts)]
    home = [
        [
            (s * experts + partner(b, d, experts), ((s + 1) % sections) * experts + b)
            for s in range(sections)
            for b in range(experts)
        ]
        for d in range(experts)
    ]

    blocks = pl.pallas_call(
        functools.partial(first_kernel, experts),
        out_shape=[block_shape] * experts,
        in_specs=[SMEM, HBM, HBM, VMEM],
        out_specs=[VMEM] * experts,
        scratch_shapes=[
            pltpu.VMEM(hidden.shape, hidden.dtype),
            pltpu.VMEM(norm_gain.shape, norm_gain.dtype),
            pltpu.SemaphoreType.DMA((2,)),
        ],
        compiler_params=pltpu.CompilerParams(vmem_limit_bytes=room(experts * capacity, width)),
        name="first_dispatch",
    )(me, hidden, norm_gain, ids)
    came_ids = lax.ppermute(ids, "section", onward)
    came_weights = lax.ppermute(weights, "section", onward)
    inner_weight, outer_weight = stage(blocks[-1], inner_weight, outer_weight)
    for tick in range(1, ticks + 1):
        arrived = [blocks[experts - 1]]
        for d in reversed(range(experts - 1)):
            arrived.insert(0, lax.ppermute(blocks[d], "expert", away[d]))
        carried = lax.ppermute(hidden, "section", onward)
        served = serve(arrived, inner_weight, outer_weight)
        returned = [
            lax.ppermute(served[d], ("section", "expert"), home[d]) for d in range(experts)
        ]
        if tick < ticks:
            hidden, *blocks = pl.pallas_call(
                functools.partial(middle_kernel, experts, tick),
                out_shape=[hidden_shape] + [block_shape] * experts,
                in_specs=[SMEM] + [VMEM] * (5 + experts),
                out_specs=[VMEM] * (1 + experts),
                compiler_params=pltpu.CompilerParams(vmem_limit_bytes=room(experts * capacity, width)),
                name="combine_dispatch",
            )(me, carried, norm_gain, ids, came_ids, came_weights, *returned)
        else:
            hidden = pl.pallas_call(
                functools.partial(last_kernel, experts, tick),
                out_shape=hidden_shape,
                in_specs=[SMEM] + [VMEM] * (3 + experts),
                out_specs=VMEM,
                compiler_params=pltpu.CompilerParams(vmem_limit_bytes=room(experts * capacity, width)),
                name="combine_last",
            )(me, carried, came_ids, came_weights, *returned)
    return hidden[None]


def solution(mesh):
    in_specs = (
        P("section", "expert", None),
        P("section", None),
        P("section", "expert", None, None),
        P("section", "expert", None, None),
        P(None, "section", "expert", None),
        P(None, "section", "expert", None),
    )
    out_specs = P("section", "expert", None)
    return jax.shard_map(
        on_device, mesh=mesh, in_specs=in_specs, out_specs=out_specs, check_vma=False
    )
```
